16 devices in a mesh: graph: 16 (over z, y, x, core).
Axes of the slice: x: 2, y: 2, z: 2, core: 2. Of those that a mesh axis runs over, the one named last changes fastest.
Arguments:
- feats: bfloat16 [32768, 500], P('graph')
- w_one: float32 [500, 256], replicated
- w_two: float32 [256, 7], replicated
- send_idx: int32 [256, 64], P('graph')
- send_count: int32 [256], P('graph')
- edge_src: int32 [32768, 12], P('graph')
- edge_wt: float32 [32768, 12], P('graph')
- labels: int32 [32768], P('graph')
- label_mask: int32 [32768], P('graph')
Outputs:
- output 1: float32 [], replicated
- output 2: float32 [500, 256], replicated
- output 3: float32 [256, 7], replicated
All inputs are finite; a program needn't handle non-finite values.
Results may differ from the reference program's by a relative error of at most 0.001.
Values are sent between devices in bfloat16 or wider.
A program may use at most 1 GiB of HBM per device.

```python
import jax
import jax.numpy as jnp
from jax import lax

GRAPH_DEVS = 16
ROWS_DEV = 2048
HALO_ROWS = 64
IN_DEG = 12
FEAT_IN = 500
FEAT_HID = 256
CLASSES = 7

TOTAL_ROWS = GRAPH_DEVS * ROWS_DEV
EXT_ROWS = ROWS_DEV + GRAPH_DEVS * HALO_ROWS


def draw_structure(rng_key):
    rng_keys = jax.random.split(rng_key, 7)
    dev_ids = jnp.arange(GRAPH_DEVS)
    skew_a = jax.random.randint(rng_keys[0], (GRAPH_DEVS, GRAPH_DEVS), 0, HALO_ROWS)
    skew_b = jax.random.randint(rng_keys[1], (GRAPH_DEVS, GRAPH_DEVS), 0, HALO_ROWS)
    counts = 1 + (skew_a * skew_b) // HALO_ROWS
    full_list = dev_ids[None, :] == (dev_ids[:, None] + 1) % GRAPH_DEVS
    counts = jnp.where(full_list, HALO_ROWS, counts)
    send_idx = jax.random.randint(rng_keys[2], (GRAPH_DEVS * GRAPH_DEVS, HALO_ROWS), 0, ROWS_DEV)
    edge_shape = (GRAPH_DEVS, ROWS_DEV, IN_DEG)
    is_cut = jax.random.randint(rng_keys[3], edge_shape, 0, 4) == 0
    local_src = jax.random.randint(rng_keys[4], edge_shape, 0, ROWS_DEV)
    peer_dev = (dev_ids[:, None, None] + jax.random.randint(rng_keys[5], edge_shape, 1, GRAPH_DEVS)) % GRAPH_DEVS
    peer_count = counts[peer_dev, dev_ids[:, None, None]]
    slot_pos = jax.random.randint(rng_keys[6], edge_shape, 0, 1048576) % peer_count
    halo_src = ROWS_DEV + peer_dev * HALO_ROWS + slot_pos
    edge_src = jnp.where(is_cut, halo_src, local_src).reshape(TOTAL_ROWS, IN_DEG)
    return send_idx, counts.reshape(GRAPH_DEVS * GRAPH_DEVS), edge_src, is_cut.reshape(TOTAL_ROWS, IN_DEG)


def setup_inputs(seed: int = 0) -> dict:
    rng_keys = jax.random.split(jax.random.key(seed), 7)
    feats = jax.random.normal(rng_keys[0], (TOTAL_ROWS, FEAT_IN), jnp.float32).astype(jnp.bfloat16)
    w_one = jax.random.normal(rng_keys[1], (FEAT_IN, FEAT_HID), jnp.float32) * FEAT_IN ** -0.5
    w_two = jax.random.normal(rng_keys[2], (FEAT_HID, CLASSES), jnp.float32) * FEAT_HID ** -0.5
    send_idx, send_count, edge_src, is_cut = draw_structure(rng_keys[3])
    raw_wt = jax.random.uniform(rng_keys[4], (TOTAL_ROWS, IN_DEG), jnp.float32, 0.5, 1.5) * jnp.where(is_cut, 0.5, 1.0)
    edge_wt = raw_wt / jnp.sqrt(jnp.sum(raw_wt * raw_wt, axis=1, keepdims=True))
    labels = jax.random.randint(rng_keys[5], (TOTAL_ROWS,), 0, CLASSES)
    label_mask = jax.random.randint(rng_keys[6], (TOTAL_ROWS,), 0, 2)
    return {"feats": feats, "w_one": w_one, "w_two": w_two, "send_idx": send_idx, "send_count": send_count, "edge_src": edge_src, "edge_wt": edge_wt, "labels": labels, "label_mask": label_mask}


def reference(feats, w_one, w_two, send_idx, send_count, edge_src, edge_wt, labels, label_mask):
    dev_ids = jnp.arange(GRAPH_DEVS)
    send_lists = send_idx.reshape(GRAPH_DEVS, GRAPH_DEVS, HALO_ROWS) + (dev_ids * ROWS_DEV)[:, None, None]
    is_valid = (jnp.arange(HALO_ROWS)[None, None, :] < send_count.reshape(GRAPH_DEVS, GRAPH_DEVS)[:, :, None]).astype(jnp.float32)
    halo_ids = jnp.transpose(send_lists, (1, 0, 2)).reshape(GRAPH_DEVS, GRAPH_DEVS * HALO_ROWS)
    halo_ok = jnp.transpose(is_valid, (1, 0, 2)).reshape(GRAPH_DEVS, GRAPH_DEVS * HALO_ROWS)
    src_dev = edge_src.reshape(GRAPH_DEVS, ROWS_DEV, IN_DEG)
    wt_dev = edge_wt.reshape(GRAPH_DEVS, ROWS_DEV, IN_DEG)

    def aggregate(h_flat):
        feat_width = h_flat.shape[1]

        def one_dev(per_dev):
            own_rows, src_ids, edge_w, ids_here, ok_here = per_dev
            halo_vals = h_flat[ids_here].astype(jnp.float32) * ok_here[:, None]
            ext_rows = jnp.concatenate([own_rows.astype(jnp.float32), halo_vals], axis=0)
            return jnp.sum(ext_rows[src_ids] * edge_w[:, :, None], axis=1)

        blocks = h_flat.reshape(GRAPH_DEVS, ROWS_DEV, feat_width)
        return lax.map(one_dev, (blocks, src_dev, wt_dev, halo_ids, halo_ok)).reshape(TOTAL_ROWS, feat_width)

    def scatter_back(d_z):
        feat_width = d_z.shape[1]

        def one_dev(per_dev):
            src_ids, edge_w, dz_rows = per_dev
            contrib = (edge_w[:, :, None] * dz_rows[:, None, :]).reshape(ROWS_DEV * IN_DEG, feat_width)
            return jax.ops.segment_sum(contrib, src_ids.reshape(ROWS_DEV * IN_DEG), num_segments=EXT_ROWS)

        ext_grad = lax.map(one_dev, (src_dev, wt_dev, d_z.reshape(GRAPH_DEVS, ROWS_DEV, feat_width)))
        own_grad = ext_grad[:, :ROWS_DEV].reshape(TOTAL_ROWS, feat_width)
        halo_grad = ext_grad[:, ROWS_DEV:] * halo_ok[:, :, None]
        back_sum = jax.ops.segment_sum(halo_grad.reshape(GRAPH_DEVS * GRAPH_DEVS * HALO_ROWS, feat_width), halo_ids.reshape(GRAPH_DEVS * GRAPH_DEVS * HALO_ROWS), num_segments=TOTAL_ROWS)
        return own_grad + back_sum

    w_one_b = w_one.astype(jnp.bfloat16)
    w_two_b = w_two.astype(jnp.bfloat16)
    z_one = aggregate(feats).astype(jnp.bfloat16)
    h_one = jnp.maximum(jnp.dot(z_one, w_one_b, preferred_element_type=jnp.float32), 0.0).astype(jnp.bfloat16)
    z_two = aggregate(h_one).astype(jnp.bfloat16)
    logits = jnp.dot(z_two, w_two_b, preferred_element_type=jnp.float32)
    mask_f = label_mask.astype(jnp.float32)
    label_total = jnp.sum(mask_f)
    log_prob = jax.nn.log_softmax(logits, axis=-1)
    onehot = (labels[:, None] == jnp.arange(CLASSES)[None, :]).astype(jnp.float32)
    loss_val = -jnp.sum(mask_f[:, None] * onehot * log_prob) / label_total
    d_logits = ((jnp.exp(log_prob) - onehot) * (mask_f / label_total)[:, None]).astype(jnp.bfloat16)
    grad_two = jnp.dot(z_two.T, d_logits, preferred_element_type=jnp.float32)
    d_z2 = jnp.dot(d_logits, w_two_b.T, preferred_element_type=jnp.float32)
    d_h1 = scatter_back(d_z2)
    d_y1 = jnp.where(h_one > 0, d_h1, 0.0).astype(jnp.bfloat16)
    grad_one = jnp.dot(z_one.T, d_y1, preferred_element_type=jnp.float32)
    return (loss_val, grad_one, grad_two)
```

```python
import functools

import jax
import jax.numpy as jnp
from jax import lax
from jax.experimental import pallas as pl
from jax.experimental.pallas import tpu as pltpu
from jax.sharding import PartitionSpec as P

DEVS = 16
ROWS = 2048
HALO = 64
DEG = 12
FIN = 500
FPAD = 512
HID = 256
CLS = 7
EXT = ROWS + DEVS * HALO
BM = 256
NB = ROWS // BM
PIECES = 3
TILES = EXT // 128
F32 = jnp.float32
BF16 = jnp.bfloat16
BIG = 3.3895313892515355e38


def split3(x):
    hi = jnp.minimum(jnp.maximum(x, -BIG), BIG).astype(BF16)
    r = x - hi.astype(F32)
    mid = r.astype(BF16)
    lo = (r - mid.astype(F32)).astype(BF16)
    return hi, mid, lo


def code_of(i):
    return jnp.left_shift(128 + jnp.bitwise_and(i, 127), jnp.right_shift(i, 7))


def kernel(feats, w1, w2, sidx, scnt, esrc, ewt, labels, lmask,
           loss_o, g1_o, g2_o,
           a3, e1, z1, e2, z2, sel, send1, send2, srcp, wtp, codes, whi, wmid, wlo, iocode, lcode,
           w1b, w2s, cnts, cnt_own, sendu, recvu, small, smallr, rt, part, rsr, red, agb, ut,
           ssem, rsem):
    me = lax.axis_index("graph")

    def peer(d):
        return lax.rem(me + d, DEVS)

    bar = pltpu.get_barrier_semaphore()
    for d in range(1, DEVS):
        pl.semaphore_signal(bar, inc=1, device_id=(peer(d),), device_id_type=pl.DeviceIdType.MESH)

    def remote(phase, d, src, dst):
        return pltpu.make_async_remote_copy(
            src_ref=src, dst_ref=dst, send_sem=ssem.at[phase, d], recv_sem=rsem.at[phase, d],
            device_id=(peer(d),), device_id_type=pl.DeviceIdType.MESH)

    lane16 = lax.broadcasted_iota(jnp.int32, (16, 128), 1)
    for t in range(TILES):
        iocode[t] = code_of(lane16 + 128 * t).astype(F32).astype(BF16)

    lcode[...] = jnp.zeros(lcode.shape, jnp.int32)
    lcode[0:DEVS, 0:HALO] = sidx[...]
    idx_t = lcode[...].T
    pos = lax.broadcasted_iota(jnp.int32, (128, 128), 0)
    cnt_l = jnp.zeros((128, 128), jnp.int32)
    lcode[0:1, 0:DEVS] = scnt[...]
    cnt_row = lcode[0:1, :]
    ok = (pos < cnt_row) & (lax.broadcasted_iota(jnp.int32, (128, 128), 1) < DEVS)
    lc = jnp.where(ok, code_of(jnp.bitwise_and(idx_t, ROWS - 1)), 0).astype(F32).astype(BF16)
    for q in range(DEVS):
        col = jnp.broadcast_to(lc[0:HALO, q:q + 1], (HALO, 128))
        for t in range(ROWS // 128):
            io = jnp.concatenate([iocode[t]] * (HALO // 16), axis=0)
            sel[q * HALO:(q + 1) * HALO, t * 128:(t + 1) * 128] = jnp.where(
                col == io, jnp.ones((HALO, 128), BF16), jnp.zeros((HALO, 128), BF16))

    e1[0:ROWS, 384:512] = jnp.zeros((ROWS, 128), BF16)
    e1[0:ROWS, 0:FIN] = feats[...]
    own = pl.multiple_of(ROWS + me * HALO, HALO)
    e1[pl.ds(own, HALO), :] = jnp.zeros((HALO, FPAD), BF16)
    e2[pl.ds(own, HALO), :] = jnp.zeros((HALO, HID), BF16)
    for b in range(4):
        send1[b * 256:(b + 1) * 256, :] = jnp.dot(
            sel[b * 256:(b + 1) * 256, :], e1[0:ROWS, :], preferred_element_type=F32).astype(BF16)
    maskf = lmask[...].astype(F32)
    cnt_own[...] = jnp.broadcast_to(jnp.sum(maskf, axis=1, keepdims=True), (8, 128))
    cnts[me] = cnt_own[...]

    pl.semaphore_wait(bar, DEVS - 1)
    first = []
    for d in range(1, DEVS):
        src = pl.multiple_of(peer(d) * HALO, HALO)
        first.append(remote(0, d, send1.at[pl.ds(src, HALO), :], e1.at[pl.ds(own, HALO), :]))
        first.append(remote(1, d, cnt_own, cnts.at[me]))
    for c in first:
        c.start()

    w1b[...] = jnp.zeros(w1b.shape, BF16)
    w1b[0:FIN, :] = w1[...].astype(BF16)
    w2s[...] = jnp.zeros(w2s.shape, F32)
    w2s[:, 0:CLS] = w2[...]
    w2t = w2s[...].T[0:8, :].astype(BF16)

    def prep(i, carry):
        r = pl.multiple_of(i * 128, 128)
        srcp[...] = jnp.full(srcp.shape, -1, jnp.int32)
        wtp[...] = jnp.zeros(wtp.shape, F32)
        srcp[:, 0:DEG] = esrc[pl.ds(r, 128), :]
        wtp[:, 0:DEG] = ewt[pl.ds(r, 128), :]
        s = srcp[...]
        w = wtp[...]
        tot = w
        for j in range(1, DEG):
            tot = tot + jnp.where(pltpu.roll(s, j, 1) == s, pltpu.roll(w, j, 1), 0.0)
        hi, mid, lo = split3(tot)
        whi[pl.ds(r, 128), :] = hi
        wmid[pl.ds(r, 128), :] = mid
        wlo[pl.ds(r, 128), :] = lo
        codes[pl.ds(r, 128), :] = jnp.where(s < 0, 0, code_of(jnp.maximum(s, 0))).astype(F32).astype(BF16)
        return carry

    lax.fori_loop(0, ROWS // 128, prep, 0)

    def build(g, carry):
        r = pl.multiple_of(g * 16, 16)
        base = pl.multiple_of((g // 16) * (BM * PIECES) + lax.rem(g, 16) * 16, 16)
        cg, hg, mg, lg = codes[pl.ds(r, 16), :], whi[pl.ds(r, 16), :], wmid[pl.ds(r, 16), :], wlo[pl.ds(r, 16), :]
        bc = [[jnp.broadcast_to(x[:, k:k + 1], (16, 128)) for k in range(DEG)] for x in (cg, hg, mg, lg)]
        for t in range(TILES):
            io = iocode[t]
            accs = [jnp.zeros((16, 128), BF16) for _ in range(PIECES)]
            for k in range(DEG):
                eq = bc[0][k] == io
                accs = [jnp.where(eq, bc[1 + p][k], accs[p]) for p in range(PIECES)]
            for p in range(PIECES):
                a3[pl.ds(pl.multiple_of(base + p * BM, 16), 16), t * 128:(t + 1) * 128] = accs[p]
        return carry

    lax.fori_loop(0, ROWS // 16, build, 0)

    for c in first:
        c.wait()

    def layer_one(i, carry):
        a = pl.multiple_of(i * BM * PIECES, BM)
        r = pl.multiple_of(i * BM, BM)
        acc = jnp.dot(a3[pl.ds(a, BM * PIECES), :], e1[...], preferred_element_type=F32)
        z = (acc[0:BM] + (acc[BM:2 * BM] + acc[2 * BM:])).astype(BF16)
        z1[pl.ds(r, BM), :] = z
        h = jnp.dot(z, w1b[...], preferred_element_type=F32)
        e2[pl.ds(r, BM), :] = jnp.maximum(h, 0.0).astype(BF16)
        return carry

    lax.fori_loop(0, NB, layer_one, 0)

    for b in range(4):
        send2[b * 256:(b + 1) * 256, :] = jnp.dot(
            sel[b * 256:(b + 1) * 256, :], e2[0:ROWS, :], preferred_element_type=F32).astype(BF16)
    second = []
    for d in range(1, DEVS):
        src = pl.multiple_of(peer(d) * HALO, HALO)
        second.append(remote(2, d, send2.at[pl.ds(src, HALO), :], e2.at[pl.ds(own, HALO), :]))
    for c in second:
        c.start()
    for c in second:
        c.wait()

    def layer_two(i, carry):
        a = pl.multiple_of(i * BM * PIECES, BM)
        r = pl.multiple_of(i * BM, BM)
        acc = jnp.dot(a3[pl.ds(a, BM * PIECES), :], e2[...], preferred_element_type=F32)
        z2[pl.ds(r, BM), :] = (acc[0:BM] + (acc[BM:2 * BM] + acc[2 * BM:])).astype(BF16)
        return carry

    lax.fori_loop(0, NB, layer_two, 0)

    nt = (((1,), (1,)), ((), ()))
    logits = lax.dot_general(w2t, z2[...], nt, preferred_element_type=F32)
    sub = lax.broadcasted_iota(jnp.int32, (8, ROWS), 0)
    logits = jnp.where(sub < CLS, logits, -BIG)
    shifted = logits - jnp.max(logits, axis=0, keepdims=True)
    expd = jnp.where(sub < CLS, jnp.exp(shifted), 0.0)
    log_prob = shifted - jnp.log(jnp.sum(expd, axis=0, keepdims=True))
    onehot = labels[...] == sub
    total = jnp.sum(cnts[...], axis=0)[0:1, 0:1]
    picked = jnp.sum(jnp.where(onehot, log_prob, 0.0), axis=0, keepdims=True)
    loss_part = jnp.sum(picked * maskf, axis=1, keepdims=True)
    prob = jnp.where(sub < CLS, jnp.exp(log_prob), 0.0)
    g2t = ((prob - onehot.astype(F32)) * (maskf / total)).astype(BF16)

    g2sum = jnp.dot(g2t, z2[...], preferred_element_type=F32)
    srow = lax.broadcasted_iota(jnp.int32, (8, HID), 0)
    small[...] = jnp.where(srow == CLS, loss_part, g2sum)
    smallr[me] = small[...]

    ut[...] = jnp.zeros(ut.shape, F32)
    for i in range(NB):
        g = g2t[:, i * BM:(i + 1) * BM]
        lhs = jnp.concatenate([g, g, g], axis=1)
        ut[...] += jnp.dot(lhs, a3[i * BM * PIECES:(i + 1) * BM * PIECES, :], preferred_element_type=F32)
    for q in range(DEVS):
        sendu[q, :, 0:HALO] = ut[:, ROWS + q * HALO:ROWS + (q + 1) * HALO]
    third = []
    for d in range(1, DEVS):
        third.append(remote(3, d, sendu.at[peer(d)], recvu.at[me]))
        third.append(remote(4, d, small, smallr.at[me]))
    recvu[me] = jnp.zeros((8, 128), F32)
    for c in third:
        c.start()
    for c in third:
        c.wait()

    for q in range(DEVS):
        rt[:, q * HALO:(q + 1) * HALO] = recvu[q, :, 0:HALO]
    pieces = jnp.concatenate([x.astype(F32) for x in split3(rt[...])], axis=0).astype(BF16)
    back = jnp.dot(pieces, sel[...], preferred_element_type=F32)
    u = ut[:, 0:ROWS] + (back[0:8] + (back[8:16] + back[16:24]))
    upieces = jnp.concatenate([x.astype(F32) for x in split3(u)], axis=0).astype(BF16)
    w2f = w2t.astype(F32)
    w2x = jnp.concatenate([w2f, w2f, w2f], axis=0).astype(BF16)
    tn = (((0,), (0,)), ((), ()))
    d_h1 = lax.dot_general(upieces, w2x, tn, preferred_element_type=F32)
    g1 = jnp.where(e2[0:ROWS, :].astype(F32) > 0, d_h1, 0.0).astype(BF16)
    part[...] = lax.dot_general(z1[...], g1, tn, preferred_element_type=F32)

    rows = FPAD // DEVS
    fourth = []
    for d in range(1, DEVS):
        src = pl.multiple_of(peer(d) * rows, rows)
        fourth.append(remote(5, d, part.at[pl.ds(src, rows), :], rsr.at[me]))
    for c in fourth:
        c.start()
    mine = pl.multiple_of(me * rows, rows)
    rsr[me] = part[pl.ds(mine, rows), :]
    for c in fourth:
        c.wait()
    red[...] = jnp.sum(rsr[...], axis=0)
    fifth = []
    for d in range(1, DEVS):
        fifth.append(remote(6, d, red, agb.at[pl.ds(mine, rows), :]))
    for c in fifth:
        c.start()
    agb[pl.ds(mine, rows), :] = red[...]
    tot = jnp.sum(smallr[...], axis=0)
    loss_o[...] = -tot[CLS:CLS + 1, 0:1] / total
    w2s[:, 0:8] = tot.T
    g2_o[...] = w2s[:, 0:CLS]
    for c in fifth:
        c.wait()
    g1_o[...] = agb[0:FIN, :]


def solution(mesh):
    def device_step(feats, w_one, w_two, send_idx, send_count, edge_src, edge_wt, labels, label_mask):
        vm = pl.BlockSpec(memory_space=pltpu.VMEM)
        loss, g1, g2 = pl.pallas_call(
            kernel,
            out_shape=(jax.ShapeDtypeStruct((1, 1), F32), jax.ShapeDtypeStruct((FIN, HID), F32),
                       jax.ShapeDtypeStruct((HID, CLS), F32)),
            in_specs=[vm] * 9,
            out_specs=(vm, vm, vm),
            scratch_shapes=[
                pltpu.VMEM((NB * BM * PIECES, EXT), BF16),
                pltpu.VMEM((EXT, FPAD), BF16),
                pltpu.VMEM((ROWS, FPAD), BF16),
                pltpu.VMEM((EXT, HID), BF16),
                pltpu.VMEM((ROWS, HID), BF16),
                pltpu.VMEM((DEVS * HALO, ROWS), BF16),
                pltpu.VMEM((DEVS * HALO, FPAD), BF16),
                pltpu.VMEM((DEVS * HALO, HID), BF16),
                pltpu.VMEM((128, 128), jnp.int32),
                pltpu.VMEM((128, 128), F32),
                pltpu.VMEM((ROWS, 128), BF16),
                pltpu.VMEM((ROWS, 128), BF16),
                pltpu.VMEM((ROWS, 128), BF16),
                pltpu.VMEM((ROWS, 128), BF16),
                pltpu.VMEM((TILES, 16, 128), BF16),
                pltpu.VMEM((128, 128), jnp.int32),
                pltpu.VMEM((FPAD, HID), BF16),
                pltpu.VMEM((HID, 128), F32),
                pltpu.VMEM((DEVS, 8, 128), F32),
                pltpu.VMEM((8, 128), F32),
                pltpu.VMEM((DEVS, 8, 128), F32),
                pltpu.VMEM((DEVS, 8, 128), F32),
                pltpu.VMEM((8, HID), F32),
                pltpu.VMEM((DEVS, 8, HID), F32),
                pltpu.VMEM((8, DEVS * HALO), F32),
                pltpu.VMEM((FPAD, HID), F32),
                pltpu.VMEM((DEVS, FPAD // DEVS, HID), F32),
                pltpu.VMEM((FPAD // DEVS, HID), F32),
                pltpu.VMEM((FPAD, HID), F32),
                pltpu.VMEM((8, EXT), F32),
                pltpu.SemaphoreType.DMA((7, DEVS)),
                pltpu.SemaphoreType.DMA((7, DEVS)),
            ],
            compiler_params=pltpu.CompilerParams(
                collective_id=0, has_side_effects=True, vmem_limit_bytes=67043328),
            name="gcn_step",
        )(feats, w_one, w_two, send_idx, send_count.reshape(1, DEVS), edge_src, edge_wt,
          labels.reshape(1, ROWS), label_mask.reshape(1, ROWS))
        return loss.reshape(()), g1, g2

    row, vec = P("graph", None), P("graph")
    return jax.shard_map(device_step, mesh=mesh, in_specs=(row, P(), P(), row, vec, row, row, vec, vec),
                         out_specs=(P(), P(), P()), check_vma=False)
```
